16 devices in a mesh: dp: 2 (over z), cp: 8 (over y, x, core).
Axes of the slice: x: 2, y: 2, z: 2, core: 2. Of those that a mesh axis runs over, the one named last changes fastest.
Arguments:
- hidden: bfloat16 [8, 2048, 6656], P('dp', 'cp')
- positions: int32 [2048], P('cp')
- w_q: bfloat16 [6656, 6656], replicated
- w_k: bfloat16 [6656, 6656], replicated
- w_v: bfloat16 [6656, 6656], replicated
- w_o: bfloat16 [6656, 6656], replicated
Outputs:
- output 1: bfloat16 [8, 2048, 6656], P('dp', 'cp')
- output 2: float32 [52], replicated
- output 3: bfloat16 [6656, 6656], replicated
- output 4: bfloat16 [6656, 6656], replicated
All inputs are finite; a program needn't handle non-finite values.
Results may differ from the reference program's by a relative error of at most 0.00771897.
Values are sent between devices in bfloat16 or wider.
A program may use at most 2.25 GiB of HBM per device.

```python
import jax
import jax.numpy as jnp
from jax import lax

BATCH_SIZE = 8
SEQ_LEN = 2048
D_MODEL = 6656
NUM_HEADS = 52
QUERY_BLOCK = 64
HEAD_DIM = 128
TAU_CLIP = 100
ROPE_THETA = 50000


def rope_rotate(tensor, pos_ids):
    half_dim = HEAD_DIM // 2
    inv_freq = jnp.float32(ROPE_THETA) ** (-jnp.arange(half_dim, dtype=jnp.float32) * (2.0 / HEAD_DIM))
    angle = pos_ids.astype(jnp.float32)[:, None] * inv_freq[None, :]
    cos_t = jnp.cos(angle)[:, None, :]
    sin_t = jnp.sin(angle)[:, None, :]
    lead_half = tensor[..., :half_dim]
    tail_half = tensor[..., half_dim:]
    return jnp.concatenate([lead_half * cos_t - tail_half * sin_t, tail_half * cos_t + lead_half * sin_t], axis=-1)


def setup_inputs(seed: int = 0) -> dict:
    root_key = jax.random.key(seed)
    sub_keys = jax.random.split(root_key, 15)
    width = NUM_HEADS * HEAD_DIM
    gaps = jax.random.randint(sub_keys[0], (SEQ_LEN,), 1, 3)
    start_pos = jax.random.randint(sub_keys[1], (), 0, SEQ_LEN // 2 + 1)
    positions = (start_pos + jnp.cumsum(gaps) - 1).astype(jnp.int32)
    spike_row = jax.random.randint(sub_keys[2], (), 0, BATCH_SIZE)
    key_slot = jax.random.randint(sub_keys[3], (), 0, SEQ_LEN // 2)
    query_slot = jax.random.randint(sub_keys[4], (), SEQ_LEN // 2, SEQ_LEN)
    clip_heads = (jax.random.permutation(sub_keys[5], NUM_HEADS) < NUM_HEADS // 2).astype(jnp.float32)
    head_gain = jax.random.uniform(sub_keys[6], (NUM_HEADS,), jnp.float32, 1.0, 1.25)
    dir_query = jax.random.normal(sub_keys[7], (D_MODEL,), jnp.float32)
    dir_query = dir_query / jnp.sqrt(jnp.sum(dir_query * dir_query))
    dir_key = jax.random.normal(sub_keys[8], (D_MODEL,), jnp.float32)
    dir_key = dir_key / jnp.sqrt(jnp.sum(dir_key * dir_key))
    plant_q = jax.random.normal(sub_keys[9], (NUM_HEADS, HEAD_DIM), jnp.float32)
    plant_q = plant_q / jnp.sqrt(jnp.mean(plant_q * plant_q, axis=-1, keepdims=True))
    plant_q = plant_q * (4.0 * head_gain * clip_heads)[:, None] * D_MODEL ** -0.5
    delta = positions[query_slot] - positions[key_slot]
    plant_k = rope_rotate(plant_q[None], delta[None])[0]
    noise_scale = 1.5 * D_MODEL ** -0.5
    w_q = noise_scale * jax.random.normal(sub_keys[10], (D_MODEL, width), jnp.float32) + dir_query[:, None] * plant_q.reshape(width)[None, :]
    w_k = noise_scale * jax.random.normal(sub_keys[11], (D_MODEL, width), jnp.float32) + dir_key[:, None] * plant_k.reshape(width)[None, :]
    w_v = jax.random.normal(sub_keys[12], (D_MODEL, width), jnp.float32) * D_MODEL ** -0.5
    w_o = jax.random.normal(sub_keys[13], (width, D_MODEL), jnp.float32) * width ** -0.5
    hidden = jax.random.normal(sub_keys[14], (BATCH_SIZE, SEQ_LEN, D_MODEL), jnp.float32)
    spike_scale = jnp.sqrt(jnp.float32(D_MODEL))
    hidden = hidden.at[spike_row, query_slot].set(spike_scale * dir_query)
    hidden = hidden.at[spike_row, key_slot].set(spike_scale * dir_key)
    return {
        "hidden": hidden.astype(jnp.bfloat16),
        "positions": positions,
        "w_q": w_q.astype(jnp.bfloat16),
        "w_k": w_k.astype(jnp.bfloat16),
        "w_v": w_v.astype(jnp.bfloat16),
        "w_o": w_o.astype(jnp.bfloat16),
    }


def reference(hidden, positions, w_q, w_k, w_v, w_o):
    score_scale = HEAD_DIM ** -0.5
    n_blocks = SEQ_LEN // QUERY_BLOCK
    pos_blocks = positions.reshape(n_blocks, QUERY_BLOCK)
    head_shape = (SEQ_LEN, NUM_HEADS, HEAD_DIM)

    def one_row(row_in):
        q_all = rope_rotate(jnp.dot(row_in, w_q, preferred_element_type=jnp.float32).reshape(head_shape), positions).astype(jnp.bfloat16)
        k_all = rope_rotate(jnp.dot(row_in, w_k, preferred_element_type=jnp.float32).reshape(head_shape), positions).astype(jnp.bfloat16)
        v_all = jnp.dot(row_in, w_v, preferred_element_type=jnp.float32).astype(jnp.bfloat16).reshape(head_shape)
        k_wide = k_all.astype(jnp.float32)
        v_wide = v_all.astype(jnp.float32)
        q_blocks = q_all.reshape(n_blocks, QUERY_BLOCK, NUM_HEADS, HEAD_DIM)

        def one_block(block_in):
            q_blk, pos_blk = block_in
            scores = jnp.einsum("qhd,khd->hqk", q_blk.astype(jnp.float32), k_wide) * score_scale
            allowed = positions[None, None, :] <= pos_blk[None, :, None]
            scores = jnp.where(allowed, scores, -jnp.inf)
            block_max = jnp.max(scores, axis=(1, 2))
            prob_w = jax.nn.softmax(scores, axis=-1)
            attn_blk = jnp.einsum("hqk,khd->qhd", prob_w, v_wide)
            return attn_blk.astype(jnp.bfloat16), block_max

        attn_blocks, block_maxes = lax.map(one_block, (q_blocks, pos_blocks))
        attn_flat = attn_blocks.reshape(SEQ_LEN, NUM_HEADS * HEAD_DIM)
        row_out = jnp.dot(attn_flat, w_o, preferred_element_type=jnp.float32).astype(jnp.bfloat16)
        return row_out, jnp.max(block_maxes, axis=0)

    attn_out, row_maxes = lax.map(one_row, hidden)
    head_max = jnp.max(row_maxes, axis=0)
    factor = jnp.where(head_max > TAU_CLIP, jnp.sqrt(TAU_CLIP / head_max), 1.0)
    col_factor = jnp.repeat(factor, HEAD_DIM)
    w_q_new = (w_q.astype(jnp.float32) * col_factor[None, :]).astype(jnp.bfloat16)
    w_k_new = (w_k.astype(jnp.float32) * col_factor[None, :]).astype(jnp.bfloat16)
    return attn_out, head_max, w_q_new, w_k_new
```

```python
import functools

import jax
import jax.numpy as jnp
from jax import lax
from jax.experimental import pallas as pl
from jax.experimental.pallas import tpu as pltpu
from jax.sharding import PartitionSpec as P


HEAD_DIM = 128
TAU_CLIP = 100.0
ROPE_THETA = 50000.0
TILE_N = 256
LOG2_E = 1.4426950408889634
VMEM_LIMIT = 62 * 1024 * 1024


def rope_tables(pos_ids):
    half_dim = HEAD_DIM // 2
    inv_freq = jnp.float32(ROPE_THETA) ** (-jnp.arange(half_dim, dtype=jnp.float32) * (2.0 / HEAD_DIM))
    angle = pos_ids.astype(jnp.float32)[:, None] * inv_freq[None, :]
    cos_t, sin_t = jnp.cos(angle), jnp.sin(angle)
    return jnp.concatenate([cos_t, cos_t], axis=-1), jnp.concatenate([-sin_t, sin_t], axis=-1)


def proj_kernel(n_chunks, n_alias, idx_ref, *refs):
    pieces = refs[: 2 * n_chunks]
    cos_ref, sin_ref, wq_ref, wk_ref, wv_ref = refs[2 * n_chunks : 2 * n_chunks + 5]
    q_ref, k_ref, v_ref, x_scr, sems = refs[2 * n_chunks + 5 + n_alias :]
    tile, chunk = pl.program_id(0), pl.program_id(1)
    rows = pieces[0].shape[0]
    core = idx_ref[0]

    def piece_copy(c, side):
        row0 = (core if side == 0 else 1 - core) * rows
        return pltpu.make_async_copy(
            pieces[2 * c + side], x_scr.at[c, pl.ds(pl.multiple_of(row0, rows), rows)], sems.at[c, side]
        )

    @pl.when(jnp.logical_and(tile == 0, chunk == 0))
    def _():
        for c in range(n_chunks):
            for side in range(2):
                piece_copy(c, side).start()

    for c in range(n_chunks):

        @pl.when(jnp.logical_and(tile == 0, chunk == c))
        def _():
            for side in range(2):
                piece_copy(c, side).wait()

    x = x_scr[chunk]
    cos_t, sin_t = cos_ref[0], sin_ref[0]
    for w_ref, o_ref in ((wq_ref, q_ref), (wk_ref, k_ref)):
        acc = jnp.dot(x, w_ref[...], preferred_element_type=jnp.float32)
        for h in range(TILE_N // HEAD_DIM):
            cols = slice(h * HEAD_DIM, (h + 1) * HEAD_DIM)
            t = acc[:, cols]
            o_ref[0, :, cols] = (t * cos_t + pltpu.roll(t, HEAD_DIM // 2, 1) * sin_t).astype(o_ref.dtype)
    v_ref[0] = jnp.dot(x, wv_ref[...], preferred_element_type=jnp.float32).astype(v_ref.dtype)


def project(idx, pieces, cos_t, sin_t, w_q, w_k, w_v, into, tile0, n_tiles):
    n_chunks = len(pieces) // 2
    rows, depth = pieces[0].shape
    total_chunks = cos_t.shape[0]
    half_cols = w_q.shape[1] // 2
    half_tiles = half_cols // TILE_N
    table_spec = pl.BlockSpec((1, 2 * rows, HEAD_DIM), lambda n, c, idx: (idx[1 + c], 0, 0))
    w_spec = pl.BlockSpec((depth, TILE_N), lambda n, c, idx: (0, idx[0] * half_tiles + tile0 + n))
    o_spec = pl.BlockSpec((1, 2 * rows, TILE_N), lambda n, c, idx: (idx[1 + c], 0, tile0 + n))
    any_spec = pl.BlockSpec(memory_space=pl.ANY)
    n_alias = 0 if into is None else 3
    o_shape = jax.ShapeDtypeStruct((total_chunks, 2 * rows, half_cols), jnp.bfloat16)
    flops = 2 * 3 * n_chunks * 2 * rows * depth * n_tiles * TILE_N
    first_alias = 1 + 2 * n_chunks + 5
    return pl.pallas_call(
        functools.partial(proj_kernel, n_chunks, n_alias),
        grid_spec=pltpu.PrefetchScalarGridSpec(
            num_scalar_prefetch=1,
            grid=(n_tiles, n_chunks),
            in_specs=[any_spec] * (2 * n_chunks) + [table_spec] * 2 + [w_spec] * 3 + [any_spec] * n_alias,
            out_specs=[o_spec] * 3,
            scratch_shapes=[
                pltpu.VMEM((n_chunks, 2 * rows, depth), jnp.bfloat16),
                pltpu.SemaphoreType.DMA((n_chunks, 2)),
            ],
        ),
        out_shape=[o_shape] * 3,
        input_output_aliases={first_alias + i: i for i in range(n_alias)},
        compiler_params=pltpu.CompilerParams(
            dimension_semantics=("arbitrary", "arbitrary"), vmem_limit_bytes=VMEM_LIMIT
        ),
        cost_estimate=pl.CostEstimate(
            flops=flops, bytes_accessed=2 * 3 * depth * n_tiles * TILE_N + 2 * n_chunks * rows * depth * 2, transcendentals=0
        ),
    )(idx, *pieces, cos_t, sin_t, w_q, w_k, w_v, *(into or ()))


def attn_kernel(blk, q_ref, k_ref, v_ref, o_ref, m_ref, s_scr):
    n_chunks, rows, _ = q_ref.shape
    per_chunk = rows // blk
    n_blocks = n_chunks * per_chunk
    scale = HEAD_DIM ** -0.5

    def rows_of(ref, i):
        r0 = (i % per_chunk) * blk
        return ref[i // per_chunk, r0 : r0 + blk, :]

    causal = lax.broadcasted_iota(jnp.int32, (blk, blk), 0) >= lax.broadcasted_iota(jnp.int32, (blk, blk), 1)
    head_max = None
    for i in range(n_blocks):
        q = rows_of(q_ref, i)
        lane_max = None
        for j in range(i + 1):
            s = lax.dot_general(q, rows_of(k_ref, j), (((1,), (1,)), ((), ())), preferred_element_type=jnp.float32)
            if j == i:
                s = jnp.where(causal, s, -jnp.inf)
            s_scr[i % 2, :, j * blk : (j + 1) * blk] = s
            for c in range(blk // HEAD_DIM):
                part = s[:, c * HEAD_DIM : (c + 1) * HEAD_DIM]
                lane_max = part if lane_max is None else jnp.maximum(lane_max, part)
        row_max = jnp.max(lane_max, axis=-1, keepdims=True)
        blk_max = jnp.max(lane_max.reshape(blk // 8, 8, HEAD_DIM), axis=0)
        head_max = blk_max if head_max is None else jnp.maximum(head_max, blk_max)
        lane_sum, acc = None, None
        for j in range(i + 1):
            p = jnp.exp2((s_scr[i % 2, :, j * blk : (j + 1) * blk] - row_max) * (scale * LOG2_E))
            for c in range(blk // HEAD_DIM):
                part = p[:, c * HEAD_DIM : (c + 1) * HEAD_DIM]
                lane_sum = part if lane_sum is None else lane_sum + part
            pv = jnp.dot(p.astype(jnp.bfloat16), rows_of(v_ref, j), preferred_element_type=jnp.float32)
            acc = pv if acc is None else acc + pv
        row_sum = jnp.sum(lane_sum, axis=-1, keepdims=True)
        r0 = (i % per_chunk) * blk
        o_ref[i // per_chunk, r0 : r0 + blk, :] = (acc / row_sum).astype(o_ref.dtype)
    m_ref[...] = head_max * scale


def attend(q, k, v, head0, n_heads):
    n_chunks, rows, _ = q.shape
    blk = min(256, rows)
    in_spec = pl.BlockSpec((n_chunks, rows, HEAD_DIM), lambda h: (0, 0, head0 + h))
    o_spec = pl.BlockSpec((n_chunks, rows, HEAD_DIM), lambda h: (0, 0, h))
    seq = n_chunks * rows
    return pl.pallas_call(
        functools.partial(attn_kernel, blk),
        grid=(n_heads,),
        in_specs=[in_spec] * 3,
        out_specs=[o_spec, pl.BlockSpec((8, HEAD_DIM), lambda h: (h, 0))],
        out_shape=[
            jax.ShapeDtypeStruct((n_chunks, rows, n_heads * HEAD_DIM), jnp.bfloat16),
            jax.ShapeDtypeStruct((8 * n_heads, HEAD_DIM), jnp.float32),
        ],
        scratch_shapes=[pltpu.VMEM((2, blk, seq), jnp.float32)],
        compiler_params=pltpu.CompilerParams(dimension_semantics=("arbitrary",), vmem_limit_bytes=VMEM_LIMIT),
        cost_estimate=pl.CostEstimate(
            flops=8 * seq * seq * HEAD_DIM * n_heads // 2,
            bytes_accessed=8 * seq * HEAD_DIM * n_heads,
            transcendentals=seq * seq * n_heads // 2,
        ),
    )(q, k, v)


def out_kernel(n_chunks, col_offs, n_alias, idx_ref, *refs):
    n_groups = len(col_offs)
    n_pieces = n_chunks * 2 * n_groups
    pieces = refs[:n_pieces]
    wo_ref, fac_ref, wc_ref = refs[n_pieces : n_pieces + 3]
    o_hbm, c_ref, a_scr, o_scr, a_sems, o_sems = refs[n_pieces + 3 + n_alias :]
    tile, n_tiles = pl.program_id(0), pl.num_programs(0)
    core = idx_ref[0]
    rows = pieces[0].shape[0]
    half_cols = a_scr.shape[1] // 2

    def piece_copies():
        copies = []
        for c in range(n_chunks):
            for side in range(2):
                for g in range(n_groups):
                    n = (c * 2 + side) * n_groups + g
                    col0 = (core if side == 0 else 1 - core) * half_cols + col_offs[g]
                    width = pieces[n].shape[1]
                    copies.append(
                        pltpu.make_async_copy(
                            pieces[n],
                            a_scr.at[pl.ds(c * rows, rows), pl.ds(pl.multiple_of(col0, HEAD_DIM), width)],
                            a_sems.at[n],
                        )
                    )
        return copies

    def out_copies(slot, at_tile):
        return [
            pltpu.make_async_copy(
                o_scr.at[slot, pl.ds(c * rows, rows)],
                o_hbm.at[idx_ref[1 + c], :, pl.ds(pl.multiple_of(at_tile * TILE_N, TILE_N), TILE_N)],
                o_sems.at[slot, c],
            )
            for c in range(n_chunks)
        ]

    @pl.when(tile == 0)
    def _():
        for copy in piece_copies():
            copy.start()
        for copy in piece_copies():
            copy.wait()

    slot = lax.rem(tile, 2)

    @pl.when(tile >= 2)
    def _():
        for copy in out_copies(slot, tile - 2):
            copy.wait()

    o_scr[slot] = jnp.dot(a_scr[...], wo_ref[...], preferred_element_type=jnp.float32).astype(o_scr.dtype)
    c_ref[...] = (wc_ref[...].astype(jnp.float32) * fac_ref[...]).astype(c_ref.dtype)
    for copy in out_copies(slot, tile):
        copy.start()

    @pl.when(tile == n_tiles - 1)
    def _():
        for copy in out_copies(1 - slot, tile - 1):
            copy.wait()
        for copy in out_copies(slot, tile):
            copy.wait()


def out_project(idx, pieces, col_offs, w_o, factor, w_clip, into, out_shape):
    n_groups = len(col_offs)
    n_chunks = len(pieces) // (2 * n_groups)
    rows = pieces[0].shape[0]
    depth, width = w_o.shape
    n_tiles = width // TILE_N
    any_spec = pl.BlockSpec(memory_space=pl.ANY)
    tile_spec = pl.BlockSpec((depth, TILE_N), lambda n, idx: (0, n))
    n_alias = 0 if into is None else 1
    alias_at = 1 + len(pieces) + 3
    return pl.pallas_call(
        functools.partial(out_kernel, n_chunks, col_offs, n_alias),
        grid_spec=pltpu.PrefetchScalarGridSpec(
            num_scalar_prefetch=1,
            grid=(n_tiles,),
            in_specs=[any_spec] * len(pieces)
            + [tile_spec, pl.BlockSpec((1, TILE_N), lambda n, idx: (0, n)), tile_spec]
            + [any_spec] * n_alias,
            out_specs=[any_spec, tile_spec],
            scratch_shapes=[
                pltpu.VMEM((n_chunks * rows, depth), jnp.bfloat16),
                pltpu.VMEM((2, n_chunks * rows, TILE_N), jnp.bfloat16),
                pltpu.SemaphoreType.DMA((len(pieces),)),
                pltpu.SemaphoreType.DMA((2, n_chunks)),
            ],
        ),
        out_shape=[jax.ShapeDtypeStruct(out_shape, jnp.bfloat16), jax.ShapeDtypeStruct(w_clip.shape, jnp.bfloat16)],
        input_output_aliases={alias_at: 0} if n_alias else {},
        compiler_params=pltpu.CompilerParams(dimension_semantics=("arbitrary",), vmem_limit_bytes=VMEM_LIMIT),
        cost_estimate=pl.CostEstimate(
            flops=2 * n_chunks * rows * depth * width, bytes_accessed=2 * 3 * depth * width, transcendentals=0
        ),
    )(idx, *pieces, w_o, factor, w_clip, *([into] if n_alias else []))


def solution(mesh):
    cp_size = mesh.shape["cp"]
    n_chips = cp_size // 2

    def permute(x, flip):
        return lax.ppermute(x, "cp", [(src, src ^ flip) for src in range(cp_size)])

    def device_body(hidden, pos_ids, w_q, w_k, w_v, w_o):
        cp_rank = lax.axis_index("cp")
        core, chip = cp_rank % 2, cp_rank // 2
        n_heads = w_q.shape[1] // HEAD_DIM
        half_heads = n_heads // 2
        half_tiles = half_heads * HEAD_DIM // TILE_N
        tiles_a = (half_tiles + 1) // 2
        heads_per_tile = TILE_N // HEAD_DIM
        groups = [(0, tiles_a), (tiles_a, half_tiles - tiles_a)]
        col_offs = tuple(t0 * TILE_N for t0, _ in groups)

        def index(*offsets):
            return jnp.stack([core] + [chip ^ d for d in offsets]).astype(jnp.int32)

        same, other = {}, {}
        for d in range(n_chips):
            row = lax.dynamic_index_in_dim(hidden, chip ^ d, 0, keepdims=False)
            same[d] = permute(row, 2 * d) if d else row
            other[d] = permute(same[d], 1)

        all_pos = lax.all_gather(pos_ids, "cp", tiled=True)
        cos_t, sin_t = (t.reshape(n_chips, -1, HEAD_DIM) for t in rope_tables(all_pos))

        def fill(qkv, offsets, tile0, n_tiles):
            pieces = [piece for d in offsets for piece in (same[d], other[d])]
            return project(index(*offsets), pieces, cos_t, sin_t, w_q, w_k, w_v, qkv, tile0, n_tiles)

        rest = tuple(range(1, n_chips))
        qkv = fill(None, (0,), 0, tiles_a)
        qkv = fill(qkv, (0,), tiles_a, half_tiles - tiles_a)
        for d in rest:
            qkv = fill(qkv, (d,), *groups[0])

        sent, maxes = [], []
        for g, (tile0, n_tiles) in enumerate(groups):
            if g == 1:
                qkv = fill(qkv, rest, tile0, n_tiles)
            vals, row_max = attend(*qkv, tile0 * heads_per_tile, n_tiles * heads_per_tile)
            maxes.append(jnp.max(row_max.reshape(n_tiles * heads_per_tile, -1), axis=1))
            vals = vals.reshape(cp_size, -1, vals.shape[-1])
            got = {}
            for d in range(n_chips):
                for side in range(2):
                    piece = lax.dynamic_index_in_dim(vals, cp_rank ^ (2 * d + side), 0, keepdims=False)
                    got[d, side] = permute(piece, 2 * d + side) if d or side else piece
            sent.append(got)

        local_max = jnp.concatenate(maxes)
        spread = jnp.full((2, half_heads), -jnp.inf, jnp.float32)
        spread = lax.dynamic_update_slice(spread, local_max[None], (core, 0)).reshape(n_heads)
        head_max = lax.pmax(spread, ("dp", "cp"))
        factor = jnp.where(head_max > TAU_CLIP, jnp.sqrt(TAU_CLIP / head_max), 1.0)
        factor = jnp.repeat(factor, HEAD_DIM)[None, :]

        def out_rows(offsets, w_clip, into):
            pieces = [sent[g][d, side] for d in offsets for side in range(2) for g in range(len(groups))]
            return out_project(index(*offsets), pieces, col_offs, w_o, factor, w_clip, into, hidden.shape)

        attn_out, w_q_new = out_rows((0,), w_q, None)
        attn_out, w_k_new = out_rows(rest, w_k, attn_out)
        return attn_out, head_max, w_q_new, w_k_new

    return jax.shard_map(
        device_body,
        mesh=mesh,
        in_specs=(P("dp", "cp", None), P("cp"), P(None, None), P(None, None), P(None, None), P(None, None)),
        out_specs=(P("dp", "cp", None), P(None), P(None, None), P(None, None)),
        check_vma=False,
    )
```

```python
import functools

import jax
import jax.numpy as jnp
from jax import lax
from jax.experimental import pallas as pl
from jax.experimental.pallas import tpu as pltpu
from jax.sharding import PartitionSpec as P


HEAD_DIM = 128
TAU_CLIP = 100.0
ROPE_THETA = 50000.0
TILE_N = 256
CLIP_ROWS = 64
LOG2_E = 1.4426950408889634
VMEM_LIMIT = 62 * 1024 * 1024


def rope_tables(pos_ids):
    half_dim = HEAD_DIM // 2
    inv_freq = jnp.float32(ROPE_THETA) ** (-jnp.arange(half_dim, dtype=jnp.float32) * (2.0 / HEAD_DIM))
    angle = pos_ids.astype(jnp.float32)[:, None] * inv_freq[None, :]
    cos_t, sin_t = jnp.cos(angle), jnp.sin(angle)
    return jnp.concatenate([cos_t, cos_t], axis=-1), jnp.concatenate([-sin_t, sin_t], axis=-1)


def clip_rows(total, n_steps):
    return -(-total // (16 * n_steps)) * 16


class ClipPass:
    def __init__(self, step, n_steps, units, fac_ref, buf, in_sems, out_sems):
        self.step, self.n_steps, self.units = step, n_steps, units
        self.fac_ref, self.buf, self.in_sems, self.out_sems = fac_ref, buf, in_sems, out_sems
        self.rows, self.width = buf.shape[2], buf.shape[3]

    def strip(self, ref, col0, step):
        row0 = pl.multiple_of(jnp.minimum(step * self.rows, ref.shape[0] - self.rows), 16)
        return ref.at[pl.ds(row0, self.rows), pl.ds(col0, self.width)]

    def copies(self, step, inward):
        slot = lax.rem(step, 3)
        for u, (src, dst, col0, _) in enumerate(self.units):
            if inward:
                yield pltpu.make_async_copy(self.strip(src, col0, step), self.buf.at[slot, u], self.in_sems.at[slot, u])
            else:
                yield pltpu.make_async_copy(self.buf.at[slot, u], self.strip(dst, col0, step), self.out_sems.at[slot, u])

    def start(self, step, inward):
        for copy in self.copies(step, inward):
            copy.start()

    def wait(self, step, inward):
        for copy in self.copies(step, inward):
            copy.wait()

    def open(self):
        step = self.step

        @pl.when(step == 0)
        def _():
            self.start(step, True)

        @pl.when(step >= 2)
        def _():
            self.wait(step - 2, False)

        @pl.when(step + 1 < self.n_steps)
        def _():
            self.start(step + 1, True)

        self.wait(step, True)

    def scale(self, u):
        slot, row = lax.rem(self.step, 3), self.units[u][3]
        for c0 in range(0, self.width, HEAD_DIM):
            fac = self.fac_ref[row : row + 1, c0 : c0 + HEAD_DIM]
            for r0 in range(0, self.rows, CLIP_ROWS):
                at = (slot, u, slice(r0, min(r0 + CLIP_ROWS, self.rows)), slice(c0, c0 + HEAD_DIM))
                self.buf[at] = (self.buf[at].astype(jnp.float32) * fac).astype(self.buf.dtype)

    def close(self):
        step = self.step
        self.start(step, False)

        @pl.when(step == self.n_steps - 1)
        def _():
            self.wait(step - 1, False)
            self.wait(step, False)


def clip_scratch(n_units, rows, width):
    return [
        pltpu.VMEM((3, n_units, rows, width), jnp.bfloat16),
        pltpu.SemaphoreType.DMA((3, n_units)),
        pltpu.SemaphoreType.DMA((3, n_units)),
    ]


def proj_kernel(n_chunks, n_alias, tile0, clip_cols, idx_ref, *refs):
    pieces = refs[: 2 * n_chunks]
    n_in = 2 * n_chunks + 5 + (1 if clip_cols else 0)
    cos_ref, sin_ref, wq_hbm, wk_hbm, wv_hbm = refs[2 * n_chunks : 2 * n_chunks + 5]
    outs = refs[n_in + n_alias :]
    (q_ref, k_ref, v_ref), outs = outs[:3], outs[3:]
    if clip_cols:
        (wq_new, wk_new), outs = outs[:2], outs[2:]
    (x_scr, x_sems, w_scr, w_sems), outs = outs[:4], outs[4:]
    tile, chunk = pl.program_id(0), pl.program_id(1)
    n_tiles = pl.num_programs(0)
    rows = pieces[0].shape[0]
    core = idx_ref[0]
    half_cols = wq_hbm.shape[1] // 2

    def piece_copy(c, side):
        row0 = (core if side == 0 else 1 - core) * rows
        return pltpu.make_async_copy(
            pieces[2 * c + side], x_scr.at[c, pl.ds(pl.multiple_of(row0, rows), rows)], x_sems.at[c, side]
        )

    def weight_copy(w, at_tile):
        col0 = pl.multiple_of(core * half_cols + (tile0 + at_tile) * TILE_N, TILE_N)
        w_hbm = (wq_hbm, wk_hbm, wv_hbm)[w]
        return pltpu.make_async_copy(w_hbm.at[:, pl.ds(col0, TILE_N)], w_scr.at[w], w_sems.at[w])

    @pl.when(jnp.logical_and(tile == 0, chunk == 0))
    def _():
        for side in range(2):
            piece_copy(0, side).start()
        for w in range(3):
            weight_copy(w, 0).start()
        for c in range(1, n_chunks):
            for side in range(2):
                piece_copy(c, side).start()

    for c in range(n_chunks):

        @pl.when(jnp.logical_and(tile == 0, chunk == c))
        def _():
            for side in range(2):
                piece_copy(c, side).wait()

    clip = None
    if clip_cols:
        units = [(src, dst, col0, h) for src, dst in ((wq_hbm, wq_new), (wk_hbm, wk_new)) for h, col0 in enumerate(clip_cols)]
        clip = ClipPass(tile * n_chunks + chunk, n_tiles * n_chunks, units, refs[2 * n_chunks + 5], *outs)
        clip.open()

    for w, o_ref in enumerate((q_ref, k_ref, v_ref)):

        @pl.when(chunk == 0)
        def _():
            weight_copy(w, tile).wait()

        acc = jnp.dot(x_scr[chunk], w_scr[w], preferred_element_type=jnp.float32)
        if w < 2:
            cos_t, sin_t = cos_ref[0], sin_ref[0]
            for h in range(TILE_N // HEAD_DIM):
                cols = slice(h * HEAD_DIM, (h + 1) * HEAD_DIM)
                t = acc[:, cols]
                o_ref[0, :, cols] = (t * cos_t + pltpu.roll(t, HEAD_DIM // 2, 1) * sin_t).astype(o_ref.dtype)
        else:
            o_ref[0] = acc.astype(o_ref.dtype)
        if clip:
            for u in range(len(clip.units)):
                if min(u, 2) == w:
                    clip.scale(u)

        @pl.when(jnp.logical_and(chunk == n_chunks - 1, tile + 1 < n_tiles))
        def _():
            weight_copy(w, tile + 1).start()

    if clip:
        clip.close()


def project(idx, pieces, cos_t, sin_t, w_q, w_k, w_v, into, tile0, n_tiles, clip_cols=(), factor=None):
    n_chunks = len(pieces) // 2
    rows, depth = pieces[0].shape
    total_chunks = cos_t.shape[0]
    half_cols = w_q.shape[1] // 2
    table_spec = pl.BlockSpec((1, 2 * rows, HEAD_DIM), lambda n, c, idx: (idx[1 + c], 0, 0))
    o_spec = pl.BlockSpec((1, 2 * rows, TILE_N), lambda n, c, idx: (idx[1 + c], 0, tile0 + n))
    any_spec = pl.BlockSpec(memory_space=pl.ANY)
    n_alias = 0 if into is None else 3
    o_shape = jax.ShapeDtypeStruct((total_chunks, 2 * rows, half_cols), jnp.bfloat16)
    flops = 2 * 3 * n_chunks * 2 * rows * depth * n_tiles * TILE_N
    first_alias = 1 + 2 * n_chunks + 5 + (1 if clip_cols else 0)
    scratch = [
        pltpu.VMEM((n_chunks, 2 * rows, depth), jnp.bfloat16),
        pltpu.SemaphoreType.DMA((n_chunks, 2)),
        pltpu.VMEM((3, depth, TILE_N), jnp.bfloat16),
        pltpu.SemaphoreType.DMA((3,)),
    ]
    clip_specs, clip_args, clip_outs = [], [], []
    if clip_cols:
        clip_specs = [pl.BlockSpec(factor.shape, lambda n, c, idx: (0, 0))]
        clip_args = [factor]
        clip_outs = [jax.ShapeDtypeStruct(w_q.shape, w_q.dtype)] * 2
        scratch += clip_scratch(2 * len(clip_cols), clip_rows(depth, n_tiles * n_chunks), factor.shape[1])
    return pl.pallas_call(
        functools.partial(proj_kernel, n_chunks, n_alias, tile0, clip_cols),
        grid_spec=pltpu.PrefetchScalarGridSpec(
            num_scalar_prefetch=1,
            grid=(n_tiles, n_chunks),
            in_specs=[any_spec] * (2 * n_chunks) + [table_spec] * 2 + [any_spec] * 3 + clip_specs + [any_spec] * n_alias,
            out_specs=[o_spec] * 3 + [any_spec] * len(clip_outs),
            scratch_shapes=scratch,
        ),
        out_shape=[o_shape] * 3 + clip_outs,
        input_output_aliases={first_alias + i: i for i in range(n_alias)},
        compiler_params=pltpu.CompilerParams(
            dimension_semantics=("arbitrary", "arbitrary"), vmem_limit_bytes=VMEM_LIMIT
        ),
        cost_estimate=pl.CostEstimate(
            flops=flops, bytes_accessed=2 * 3 * depth * n_tiles * TILE_N + 2 * n_chunks * rows * depth * 2, transcendentals=0
        ),
    )(idx, *pieces, cos_t, sin_t, w_q, w_k, w_v, *clip_args, *(into or ()))


def attn_kernel(blk, q_ref, k_ref, v_ref, o_ref, m_ref, s_scr, p_scr):
    n_chunks, rows, _ = q_ref.shape
    per_chunk = rows // blk
    n_blocks = n_chunks * per_chunk
    scale = HEAD_DIM ** -0.5
    lanes = blk // HEAD_DIM if blk >= HEAD_DIM else 1
    width = blk // lanes
    causal = lax.broadcasted_iota(jnp.int32, (blk, blk), 0) >= lax.broadcasted_iota(jnp.int32, (blk, blk), 1)

    def rows_of(ref, i):
        r0 = (i % per_chunk) * blk
        return ref[i // per_chunk, r0 : r0 + blk, :]

    def scores(i):
        q = rows_of(q_ref, i)
        lane_max = None
        for j in range(i + 1):
            s = lax.dot_general(q, rows_of(k_ref, j), (((1,), (1,)), ((), ())), preferred_element_type=jnp.float32)
            if j == i:
                s = jnp.where(causal, s, -jnp.inf)
            s_scr[i % 2, :, j * blk : (j + 1) * blk] = s
            for c in range(lanes):
                part = s[:, c * width : (c + 1) * width]
                lane_max = part if lane_max is None else jnp.maximum(lane_max, part)
        return jnp.max(lane_max, axis=-1, keepdims=True)

    row_max = scores(0)
    head_max = row_max
    for i in range(n_blocks):
        if i + 1 < n_blocks:
            next_max = scores(i + 1)
            head_max = jnp.maximum(head_max, next_max)
        lane_sum = None
        for j in range(i + 1):
            cols = slice(j * blk, (j + 1) * blk)
            p = jnp.exp2((s_scr[i % 2, :, cols] - row_max) * (scale * LOG2_E))
            for c in range(lanes):
                part = p[:, c * width : (c + 1) * width]
                lane_sum = part if lane_sum is None else lane_sum + part
            p_scr[i % 2, :, cols] = p.astype(p_scr.dtype)
        keys = (i + 1) * blk
        values = v_ref[...].reshape(n_chunks * rows, HEAD_DIM)[:keys]
        acc = jnp.dot(p_scr[i % 2, :, :keys], values, preferred_element_type=jnp.float32)
        row_sum = jnp.sum(lane_sum, axis=-1, keepdims=True)
        r0 = (i % per_chunk) * blk
        o_ref[i // per_chunk, r0 : r0 + blk, :] = (acc / row_sum).astype(o_ref.dtype)
        if i + 1 < n_blocks:
            row_max = next_max
    m_ref[...] = jnp.broadcast_to(jnp.max(head_max, axis=0, keepdims=True) * scale, m_ref.shape)


def attend(q, k, v, head0, n_heads):
    n_chunks, rows, _ = q.shape
    blk = min(256, rows)
    in_spec = pl.BlockSpec((n_chunks, rows, HEAD_DIM), lambda h: (0, 0, head0 + h))
    o_spec = pl.BlockSpec((n_chunks, rows, HEAD_DIM), lambda h: (0, 0, h))
    seq = n_chunks * rows
    return pl.pallas_call(
        functools.partial(attn_kernel, blk),
        grid=(n_heads,),
        in_specs=[in_spec] * 3,
        out_specs=[o_spec, pl.BlockSpec((8, HEAD_DIM), lambda h: (h, 0))],
        out_shape=[
            jax.ShapeDtypeStruct((n_chunks, rows, n_heads * HEAD_DIM), jnp.bfloat16),
            jax.ShapeDtypeStruct((8 * n_heads, HEAD_DIM), jnp.float32),
        ],
        scratch_shapes=[pltpu.VMEM((2, blk, seq), jnp.float32), pltpu.VMEM((2, blk, seq), jnp.bfloat16)],
        compiler_params=pltpu.CompilerParams(dimension_semantics=("arbitrary",), vmem_limit_bytes=VMEM_LIMIT),
        cost_estimate=pl.CostEstimate(
            flops=8 * seq * seq * HEAD_DIM * n_heads // 2,
            bytes_accessed=8 * seq * HEAD_DIM * n_heads,
            transcendentals=seq * seq * n_heads // 2,
        ),
    )(q, k, v)


def out_kernel(n_chunks, col_offs, n_alias, clip_cols, idx_ref, *refs):
    n_groups = len(col_offs)
    n_pieces = n_chunks * 2 * n_groups
    pieces = refs[:n_pieces]
    wo_ref, fac_ref, wc_hbm = refs[n_pieces : n_pieces + 3]
    o_hbm, c_hbm, a_scr, o_scr, a_sems, o_sems, *clip_refs = refs[n_pieces + 3 + n_alias :]
    tile, n_tiles = pl.program_id(0), pl.num_programs(0)
    core = idx_ref[0]
    rows = pieces[0].shape[0]
    half_cols = a_scr.shape[1] // 2

    def piece_copies():
        copies = []
        for c in range(n_chunks):
            for side in range(2):
                for g in range(n_groups):
                    n = (c * 2 + side) * n_groups + g
                    col0 = (core if side == 0 else 1 - core) * half_cols + col_offs[g]
                    width = pieces[n].shape[1]
                    copies.append(
                        pltpu.make_async_copy(
                            pieces[n],
                            a_scr.at[pl.ds(c * rows, rows), pl.ds(pl.multiple_of(col0, HEAD_DIM), width)],
                            a_sems.at[n],
                        )
                    )
        return copies

    def out_copies(slot, at_tile):
        return [
            pltpu.make_async_copy(
                o_scr.at[slot, pl.ds(c * rows, rows)],
                o_hbm.at[idx_ref[1 + c], :, pl.ds(pl.multiple_of(at_tile * TILE_N, TILE_N), TILE_N)],
                o_sems.at[slot, c],
            )
            for c in range(n_chunks)
        ]

    @pl.when(tile == 0)
    def _():
        for copy in piece_copies():
            copy.start()

    clip = ClipPass(tile, n_tiles, [(wc_hbm, c_hbm, col0, h) for h, col0 in enumerate(clip_cols)], fac_ref, *clip_refs)
    clip.open()

    @pl.when(tile == 0)
    def _():
        for copy in piece_copies():
            copy.wait()

    slot = lax.rem(tile, 2)

    @pl.when(tile >= 2)
    def _():
        for copy in out_copies(slot, tile - 2):
            copy.wait()

    o_scr[slot] = jnp.dot(a_scr[...], wo_ref[...], preferred_element_type=jnp.float32).astype(o_scr.dtype)
    for u in range(len(clip.units)):
        clip.scale(u)
    for copy in out_copies(slot, tile):
        copy.start()
    clip.close()

    @pl.when(tile == n_tiles - 1)
    def _():
        for copy in out_copies(1 - slot, tile - 1):
            copy.wait()
        for copy in out_copies(slot, tile):
            copy.wait()


def out_project(idx, pieces, col_offs, w_o, factor, w_clip, clip_into, clip_cols, into, out_shape):
    n_groups = len(col_offs)
    n_chunks = len(pieces) // (2 * n_groups)
    rows = pieces[0].shape[0]
    depth, width = w_o.shape
    n_tiles = width // TILE_N
    any_spec = pl.BlockSpec(memory_space=pl.ANY)
    tile_spec = pl.BlockSpec((depth, TILE_N), lambda n, idx: (0, n))
    alias_at = 1 + len(pieces) + 3
    aliased, aliases = [clip_into], {alias_at: 1}
    if into is not None:
        aliased, aliases = [clip_into, into], {alias_at: 1, alias_at + 1: 0}
    return pl.pallas_call(
        functools.partial(out_kernel, n_chunks, col_offs, len(aliased), clip_cols),
        grid_spec=pltpu.PrefetchScalarGridSpec(
            num_scalar_prefetch=1,
            grid=(n_tiles,),
            in_specs=[any_spec] * len(pieces)
            + [tile_spec, pl.BlockSpec(factor.shape, lambda n, idx: (0, 0)), any_spec]
            + [any_spec] * len(aliased),
            out_specs=[any_spec, any_spec],
            scratch_shapes=[
                pltpu.VMEM((n_chunks * rows, depth), jnp.bfloat16),
                pltpu.VMEM((2, n_chunks * rows, TILE_N), jnp.bfloat16),
                pltpu.SemaphoreType.DMA((len(pieces),)),
                pltpu.SemaphoreType.DMA((2, n_chunks)),
            ]
            + clip_scratch(len(clip_cols), clip_rows(w_clip.shape[0], n_tiles), factor.shape[1]),
        ),
        out_shape=[jax.ShapeDtypeStruct(out_shape, jnp.bfloat16), jax.ShapeDtypeStruct(w_clip.shape, jnp.bfloat16)],
        input_output_aliases=aliases,
        compiler_params=pltpu.CompilerParams(dimension_semantics=("arbitrary",), vmem_limit_bytes=VMEM_LIMIT),
        cost_estimate=pl.CostEstimate(
            flops=2 * n_chunks * rows * depth * width, bytes_accessed=2 * 2 * depth * width, transcendentals=0
        ),
    )(idx, *pieces, w_o, factor, w_clip, *aliased)


def solution(mesh):
    cp_size = mesh.shape["cp"]
    n_chips = cp_size // 2

    def permute(x, flip):
        return lax.ppermute(x, "cp", [(src, src ^ flip) for src in range(cp_size)])

    def device_body(hidden, pos_ids, w_q, w_k, w_v, w_o):
        cp_rank = lax.axis_index("cp")
        core, chip = cp_rank % 2, cp_rank // 2
        n_heads = w_q.shape[1] // HEAD_DIM
        half_heads = n_heads // 2
        half_tiles = half_heads * HEAD_DIM // TILE_N
        tiles_a = (half_tiles + 1) // 2
        heads_per_tile = TILE_N // HEAD_DIM
        groups = [(0, tiles_a), (tiles_a, half_tiles - tiles_a)]
        col_offs = tuple(t0 * TILE_N for t0, _ in groups)

        def index(*offsets):
            return jnp.stack([core] + [chip ^ d for d in offsets]).astype(jnp.int32)

        all_pos = lax.all_gather(pos_ids, "cp", tiled=True)
        cos_t, sin_t = (t.reshape(n_chips, -1, HEAD_DIM) for t in rope_tables(all_pos))

        same, other = {}, {}
        for d in range(n_chips):
            row = lax.dynamic_index_in_dim(hidden, chip ^ d, 0, keepdims=False)
            same[d] = permute(row, 2 * d) if d else row
            other[d] = permute(same[d], 1)

        def fill(qkv, offsets, tile0, n_tiles, *clip):
            pieces = [piece for d in offsets for piece in (same[d], other[d])]
            return project(index(*offsets), pieces, cos_t, sin_t, w_q, w_k, w_v, qkv, tile0, n_tiles, *clip)

        rest = tuple(range(1, n_chips))
        split = half_tiles - max(half_tiles // 4, 1)
        qkv = fill(None, (0,), 0, split)
        qkv = fill(qkv, (0,), split, half_tiles - split)
        qkv = fill(qkv, rest[:-1], *groups[0])
        qkv = fill(qkv, rest[-1:], *groups[0])

        sent, maxes, factors, clip_cols = [], [], [], []
        for g, (tile0, n_tiles) in enumerate(groups):
            n_group = n_tiles * heads_per_tile
            if g == 1:
                *qkv, w_q_new, w_k_new = fill(qkv, rest, tile0, n_tiles, clip_cols[0], factors[0])
            vals, row_max = attend(*qkv, tile0 * heads_per_tile, n_group)
            local_max = jnp.max(row_max.reshape(n_group, -1), axis=1)
            spread = jnp.where(jnp.arange(2)[:, None] == core, local_max[None, :], -jnp.inf)
            group_max = lax.pmax(spread, ("dp", "cp"))
            maxes.append(group_max)
            factor = jnp.where(group_max > TAU_CLIP, jnp.sqrt(TAU_CLIP / group_max), 1.0)
            factors.append(jnp.repeat(factor, HEAD_DIM, axis=1))
            clip_cols.append(tuple((h * half_tiles + tile0) * TILE_N for h in range(2)))
            vals = vals.reshape(cp_size, -1, vals.shape[-1])
            got = {}
            for d in range(n_chips):
                for side in range(2):
                    piece = lax.dynamic_index_in_dim(vals, cp_rank ^ (2 * d + side), 0, keepdims=False)
                    got[d, side] = permute(piece, 2 * d + side) if d or side else piece
            sent.append(got)
        head_max = jnp.concatenate(maxes, axis=1).reshape(n_heads)

        def out_rows(offsets, w_clip, clip_into, into):
            pieces = [sent[g][d, side] for d in offsets for side in range(2) for g in range(len(groups))]
            return out_project(
                index(*offsets), pieces, col_offs, w_o, factors[1], w_clip, clip_into, clip_cols[1], into, hidden.shape
            )

        attn_out, w_q_new = out_rows((0,), w_q, w_q_new, None)
        attn_out, w_k_new = out_rows(rest, w_k, w_k_new, attn_out)
        return attn_out, head_max, w_q_new, w_k_new

    return jax.shard_map(
        device_body,
        mesh=mesh,
        in_specs=(P("dp", "cp", None), P("cp"), P(None, None), P(None, None), P(None, None), P(None, None)),
        out_specs=(P("dp", "cp", None), P(None), P(None, None), P(None, None)),
        check_vma=False,
    )
```

```python
import functools

import jax
import jax.numpy as jnp
from jax import lax
from jax.experimental import pallas as pl
from jax.experimental.pallas import tpu as pltpu
from jax.sharding import PartitionSpec as P


HEAD_DIM = 128
TAU_CLIP = 100.0
ROPE_THETA = 50000.0
TILE_N = 256
OUT_N = 512
CLIP_ROWS = 64
LOG2_E = 1.4426950408889634
VMEM_LIMIT = 67043328


def rope_tables(pos_ids):
    half_dim = HEAD_DIM // 2
    inv_freq = jnp.float32(ROPE_THETA) ** (-jnp.arange(half_dim, dtype=jnp.float32) * (2.0 / HEAD_DIM))
    angle = pos_ids.astype(jnp.float32)[:, None] * inv_freq[None, :]
    cos_t, sin_t = jnp.cos(angle), jnp.sin(angle)
    return jnp.concatenate([cos_t, cos_t], axis=-1), jnp.concatenate([-sin_t, sin_t], axis=-1)


def clip_rows(total, n_steps):
    return -(-total // (16 * n_steps)) * 16


class ClipPass:
    def __init__(self, step, n_steps, units, fac_ref, buf, in_sems, out_sems):
        self.step, self.n_steps, self.units = step, n_steps, units
        self.fac_ref, self.buf, self.in_sems, self.out_sems = fac_ref, buf, in_sems, out_sems
        self.rows, self.width = buf.shape[2], buf.shape[3]

    def strip(self, ref, col0, step):
        row0 = pl.multiple_of(jnp.minimum(step * self.rows, ref.shape[0] - self.rows), 16)
        return ref.at[pl.ds(row0, self.rows), pl.ds(col0, self.width)]

    def copies(self, step, inward):
        slot = lax.rem(step, 3)
        for u, (src, dst, col0, _) in enumerate(self.units):
            if inward:
                yield pltpu.make_async_copy(self.strip(src, col0, step), self.buf.at[slot, u], self.in_sems.at[slot, u])
            else:
                yield pltpu.make_async_copy(self.buf.at[slot, u], self.strip(dst, col0, step), self.out_sems.at[slot, u])

    def start(self, step, inward):
        for copy in self.copies(step, inward):
            copy.start()

    def wait(self, step, inward):
        for copy in self.copies(step, inward):
            copy.wait()

    def open(self):
        step = self.step

        @pl.when(step == 0)
        def _():
            self.start(step, True)

        @pl.when(step >= 2)
        def _():
            self.wait(step - 2, False)

        @pl.when(step + 1 < self.n_steps)
        def _():
            self.start(step + 1, True)

        self.wait(step, True)

    def scale(self, u):
        slot, row = lax.rem(self.step, 3), self.units[u][3]
        for c0 in range(0, self.width, HEAD_DIM):
            fac = self.fac_ref[row : row + 1, c0 : c0 + HEAD_DIM]
            for r0 in range(0, self.rows, CLIP_ROWS):
                at = (slot, u, slice(r0, min(r0 + CLIP_ROWS, self.rows)), slice(c0, c0 + HEAD_DIM))
                self.buf[at] = (self.buf[at].astype(jnp.float32) * fac).astype(self.buf.dtype)

    def close(self):
        step = self.step
        self.start(step, False)

        @pl.when(step == self.n_steps - 1)
        def _():
            self.wait(step - 1, False)
            self.wait(step, False)


def clip_scratch(n_units, rows, width):
    return [
        pltpu.VMEM((3, n_units, rows, width), jnp.bfloat16),
        pltpu.SemaphoreType.DMA((3, n_units)),
        pltpu.SemaphoreType.DMA((3, n_units)),
    ]


def proj_kernel(n_chunks, n_alias, tile0, clip_cols, idx_ref, *refs):
    pieces = refs[: 2 * n_chunks]
    n_in = 2 * n_chunks + 5 + (1 if clip_cols else 0)
    cos_ref, sin_ref, wq_hbm, wk_hbm, wv_hbm = refs[2 * n_chunks : 2 * n_chunks + 5]
    outs = refs[n_in + n_alias :]
    (q_ref, k_ref, v_ref), outs = outs[:3], outs[3:]
    if clip_cols:
        (wq_new, wk_new), outs = outs[:2], outs[2:]
    (x_scr, x_sems, w_scr, w_sems), outs = outs[:4], outs[4:]
    tile, chunk = pl.program_id(0), pl.program_id(1)
    n_tiles = pl.num_programs(0)
    rows = pieces[0].shape[0]
    core = idx_ref[0]
    half_cols = wq_hbm.shape[1] // 2

    def piece_copy(c, side):
        row0 = (core if side == 0 else 1 - core) * rows
        return pltpu.make_async_copy(
            pieces[2 * c + side], x_scr.at[c, pl.ds(pl.multiple_of(row0, rows), rows)], x_sems.at[c, side]
        )

    def weight_copy(w, at_tile):
        col0 = pl.multiple_of(core * half_cols + (tile0 + at_tile) * TILE_N, TILE_N)
        w_hbm, slot = (wq_hbm, wk_hbm, wv_hbm)[w], lax.rem(at_tile, 2)
        return pltpu.make_async_copy(w_hbm.at[:, pl.ds(col0, TILE_N)], w_scr.at[slot, w], w_sems.at[slot, w])

    @pl.when(jnp.logical_and(tile == 0, chunk == 0))
    def _():
        for side in range(2):
            piece_copy(0, side).start()
        for w in range(3):
            weight_copy(w, 0).start()
        for c in range(1, n_chunks):
            for side in range(2):
                piece_copy(c, side).start()

    for c in range(n_chunks):

        @pl.when(jnp.logical_and(tile == 0, chunk == c))
        def _():
            for side in range(2):
                piece_copy(c, side).wait()

    clip = None
    if clip_cols:
        units = [(src, dst, col0, h) for src, dst in ((wq_hbm, wq_new), (wk_hbm, wk_new)) for h, col0 in enumerate(clip_cols)]
        clip = ClipPass(tile * n_chunks + chunk, n_tiles * n_chunks, units, refs[2 * n_chunks + 5], *outs)
        clip.open()

    @pl.when(chunk == 0)
    def _():
        @pl.when(tile + 1 < n_tiles)
        def _():
            for w in range(3):
                weight_copy(w, tile + 1).start()

        for w in range(3):
            weight_copy(w, tile).wait()

    slot = lax.rem(tile, 2)
    x = x_scr[chunk]
    for w, o_ref in enumerate((q_ref, k_ref, v_ref)):
        acc = jnp.dot(x, w_scr[slot, w], preferred_element_type=jnp.float32)
        if w < 2:
            cos_t, sin_t = cos_ref[0], sin_ref[0]
            for h in range(TILE_N // HEAD_DIM):
                cols = slice(h * HEAD_DIM, (h + 1) * HEAD_DIM)
                t = acc[:, cols]
                o_ref[0, :, cols] = (t * cos_t + pltpu.roll(t, HEAD_DIM // 2, 1) * sin_t).astype(o_ref.dtype)
        else:
            o_ref[0] = acc.astype(o_ref.dtype)
        if clip:
            for u in range(len(clip.units)):
                if min(u, 2) == w:
                    clip.scale(u)

    if clip:
        clip.close()


def project(idx, pieces, cos_t, sin_t, w_q, w_k, w_v, into, tile0, n_tiles, clip_cols=(), factor=None):
    n_chunks = len(pieces) // 2
    rows, depth = pieces[0].shape
    total_chunks = cos_t.shape[0]
    half_cols = w_q.shape[1] // 2
    table_spec = pl.BlockSpec((1, 2 * rows, HEAD_DIM), lambda n, c, idx: (idx[1 + c], 0, 0))
    o_spec = pl.BlockSpec((1, 2 * rows, TILE_N), lambda n, c, idx: (idx[1 + c], 0, tile0 + n))
    any_spec = pl.BlockSpec(memory_space=pl.ANY)
    n_alias = 0 if into is None else 3
    o_shape = jax.ShapeDtypeStruct((total_chunks, 2 * rows, half_cols), jnp.bfloat16)
    flops = 2 * 3 * n_chunks * 2 * rows * depth * n_tiles * TILE_N
    first_alias = 1 + 2 * n_chunks + 5 + (1 if clip_cols else 0)
    scratch = [
        pltpu.VMEM((n_chunks, 2 * rows, depth), jnp.bfloat16),
        pltpu.SemaphoreType.DMA((n_chunks, 2)),
        pltpu.VMEM((2, 3, depth, TILE_N), jnp.bfloat16),
        pltpu.SemaphoreType.DMA((2, 3)),
    ]
    clip_specs, clip_args, clip_outs = [], [], []
    if clip_cols:
        clip_specs = [pl.BlockSpec(factor.shape, lambda n, c, idx: (0, 0))]
        clip_args = [factor]
        clip_outs = [jax.ShapeDtypeStruct(w_q.shape, w_q.dtype)] * 2
        scratch += clip_scratch(2 * len(clip_cols), clip_rows(depth, n_tiles * n_chunks), factor.shape[1])
    return pl.pallas_call(
        functools.partial(proj_kernel, n_chunks, n_alias, tile0, clip_cols),
        grid_spec=pltpu.PrefetchScalarGridSpec(
            num_scalar_prefetch=1,
            grid=(n_tiles, n_chunks),
            in_specs=[any_spec] * (2 * n_chunks) + [table_spec] * 2 + [any_spec] * 3 + clip_specs + [any_spec] * n_alias,
            out_specs=[o_spec] * 3 + [any_spec] * len(clip_outs),
            scratch_shapes=scratch,
        ),
        out_shape=[o_shape] * 3 + clip_outs,
        input_output_aliases={first_alias + i: i for i in range(n_alias)},
        compiler_params=pltpu.CompilerParams(
            dimension_semantics=("arbitrary", "arbitrary"), vmem_limit_bytes=VMEM_LIMIT
        ),
        cost_estimate=pl.CostEstimate(
            flops=flops, bytes_accessed=2 * 3 * depth * n_tiles * TILE_N + 2 * n_chunks * rows * depth * 2, transcendentals=0
        ),
    )(idx, *pieces, cos_t, sin_t, w_q, w_k, w_v, *clip_args, *(into or ()))


def attn_kernel(blk, q_ref, k_ref, v_ref, o_ref, m_ref, s_scr, p_scr):
    n_chunks, rows, _ = q_ref.shape
    per_chunk = rows // blk
    n_blocks = n_chunks * per_chunk
    scale = HEAD_DIM ** -0.5
    lanes = blk // HEAD_DIM if blk >= HEAD_DIM else 1
    width = blk // lanes
    causal = lax.broadcasted_iota(jnp.int32, (blk, blk), 0) >= lax.broadcasted_iota(jnp.int32, (blk, blk), 1)

    def rows_of(ref, i):
        r0 = (i % per_chunk) * blk
        return ref[i // per_chunk, r0 : r0 + blk, :]

    def scores(i):
        q = rows_of(q_ref, i)
        lane_max = None
        for j in range(i + 1):
            s = lax.dot_general(q, rows_of(k_ref, j), (((1,), (1,)), ((), ())), preferred_element_type=jnp.float32)
            if j == i:
                s = jnp.where(causal, s, -jnp.inf)
            s_scr[i % 2, :, j * blk : (j + 1) * blk] = s
            for c in range(lanes):
                part = s[:, c * width : (c + 1) * width]
                lane_max = part if lane_max is None else jnp.maximum(lane_max, part)
        return jnp.max(lane_max, axis=-1, keepdims=True)

    row_max = scores(0)
    head_max = row_max
    for i in range(n_blocks):
        if i + 1 < n_blocks:
            next_max = scores(i + 1)
            head_max = jnp.maximum(head_max, next_max)
        lane_sum = None
        for j in range(i + 1):
            cols = slice(j * blk, (j + 1) * blk)
            p = jnp.exp2((s_scr[i % 2, :, cols] - row_max) * (scale * LOG2_E))
            for c in range(lanes):
                part = p[:, c * width : (c + 1) * width]
                lane_sum = part if lane_sum is None else lane_sum + part
            p_scr[i % 2, :, cols] = p.astype(p_scr.dtype)
        keys = (i + 1) * blk
        values = v_ref[...].reshape(n_chunks * rows, HEAD_DIM)[:keys]
        acc = jnp.dot(p_scr[i % 2, :, :keys], values, preferred_element_type=jnp.float32)
        row_sum = jnp.sum(lane_sum, axis=-1, keepdims=True)
        r0 = (i % per_chunk) * blk
        o_ref[i // per_chunk, r0 : r0 + blk, :] = (acc / row_sum).astype(o_ref.dtype)
        if i + 1 < n_blocks:
            row_max = next_max
    m_ref[...] = jnp.broadcast_to(jnp.max(head_max, axis=0, keepdims=True) * scale, m_ref.shape)


def attend(q, k, v, head0, n_heads):
    n_chunks, rows, _ = q.shape
    blk = min(256, rows)
    in_spec = pl.BlockSpec((n_chunks, rows, HEAD_DIM), lambda h: (0, 0, head0 + h))
    o_spec = pl.BlockSpec((n_chunks, rows, HEAD_DIM), lambda h: (0, 0, h))
    seq = n_chunks * rows
    return pl.pallas_call(
        functools.partial(attn_kernel, blk),
        grid=(n_heads,),
        in_specs=[in_spec] * 3,
        out_specs=[o_spec, pl.BlockSpec((8, HEAD_DIM), lambda h: (h, 0))],
        out_shape=[
            jax.ShapeDtypeStruct((n_chunks, rows, n_heads * HEAD_DIM), jnp.bfloat16),
            jax.ShapeDtypeStruct((8 * n_heads, HEAD_DIM), jnp.float32),
        ],
        scratch_shapes=[pltpu.VMEM((2, blk, seq), jnp.float32), pltpu.VMEM((2, blk, seq), jnp.bfloat16)],
        compiler_params=pltpu.CompilerParams(dimension_semantics=("arbitrary",), vmem_limit_bytes=VMEM_LIMIT),
        cost_estimate=pl.CostEstimate(
            flops=8 * seq * seq * HEAD_DIM * n_heads // 2,
            bytes_accessed=8 * seq * HEAD_DIM * n_heads,
            transcendentals=seq * seq * n_heads // 2,
        ),
    )(q, k, v)


def out_kernel(n_chunks, col_offs, n_alias, clip_cols, idx_ref, *refs):
    n_groups = len(col_offs)
    n_pieces = n_chunks * 2 * n_groups
    pieces = refs[:n_pieces]
    wo_ref, fac_ref, wc_hbm = refs[n_pieces : n_pieces + 3]
    o_hbm, c_hbm, a_scr, o_scr, a_sems, o_sems, *clip_refs = refs[n_pieces + 3 + n_alias :]
    tile, n_tiles = pl.program_id(0), pl.num_programs(0)
    core = idx_ref[0]
    rows = pieces[0].shape[0]
    half_cols = a_scr.shape[1] // 2

    def piece_copies():
        copies = []
        for c in range(n_chunks):
            for side in range(2):
                for g in range(n_groups):
                    n = (c * 2 + side) * n_groups + g
                    col0 = (core if side == 0 else 1 - core) * half_cols + col_offs[g]
                    width = pieces[n].shape[1]
                    copies.append(
                        pltpu.make_async_copy(
                            pieces[n],
                            a_scr.at[pl.ds(c * rows, rows), pl.ds(pl.multiple_of(col0, HEAD_DIM), width)],
                            a_sems.at[n],
                        )
                    )
        return copies

    def out_copies(slot, at_tile):
        return [
            pltpu.make_async_copy(
                o_scr.at[slot, pl.ds(c * rows, rows)],
                o_hbm.at[idx_ref[1 + c], :, pl.ds(pl.multiple_of(at_tile * OUT_N, OUT_N), OUT_N)],
                o_sems.at[slot, c],
            )
            for c in range(n_chunks)
        ]

    @pl.when(tile == 0)
    def _():
        for copy in piece_copies():
            copy.start()

    clip = ClipPass(tile, n_tiles, [(wc_hbm, c_hbm, col0, h) for h, col0 in enumerate(clip_cols)], fac_ref, *clip_refs)
    clip.open()

    @pl.when(tile == 0)
    def _():
        for copy in piece_copies():
            copy.wait()

    slot = lax.rem(tile, 2)

    @pl.when(tile >= 2)
    def _():
        for copy in out_copies(slot, tile - 2):
            copy.wait()

    a = a_scr[...]
    for c0 in range(0, OUT_N, TILE_N):
        cols = slice(c0, c0 + TILE_N)
        o_scr[slot, :, cols] = jnp.dot(a, wo_ref[:, cols], preferred_element_type=jnp.float32).astype(o_scr.dtype)
    for u in range(len(clip.units)):
        clip.scale(u)
    for copy in out_copies(slot, tile):
        copy.start()
    clip.close()

    @pl.when(tile == n_tiles - 1)
    def _():
        for copy in out_copies(1 - slot, tile - 1):
            copy.wait()
        for copy in out_copies(slot, tile):
            copy.wait()


def out_project(idx, pieces, col_offs, w_o, factor, w_clip, clip_into, clip_cols, into, out_shape):
    n_groups = len(col_offs)
    n_chunks = len(pieces) // (2 * n_groups)
    rows = pieces[0].shape[0]
    depth, width = w_o.shape
    n_tiles = width // OUT_N
    any_spec = pl.BlockSpec(memory_space=pl.ANY)
    tile_spec = pl.BlockSpec((depth, OUT_N), lambda n, idx: (0, n))
    alias_at = 1 + len(pieces) + 3
    aliased, aliases = [clip_into], {alias_at: 1}
    if into is not None:
        aliased, aliases = [clip_into, into], {alias_at: 1, alias_at + 1: 0}
    return pl.pallas_call(
        functools.partial(out_kernel, n_chunks, col_offs, len(aliased), clip_cols),
        grid_spec=pltpu.PrefetchScalarGridSpec(
            num_scalar_prefetch=1,
            grid=(n_tiles,),
            in_specs=[any_spec] * len(pieces)
            + [tile_spec, pl.BlockSpec(factor.shape, lambda n, idx: (0, 0)), any_spec]
            + [any_spec] * len(aliased),
            out_specs=[any_spec, any_spec],
            scratch_shapes=[
                pltpu.VMEM((n_chunks * rows, depth), jnp.bfloat16),
                pltpu.VMEM((2, n_chunks * rows, OUT_N), jnp.bfloat16),
                pltpu.SemaphoreType.DMA((len(pieces),)),
                pltpu.SemaphoreType.DMA((2, n_chunks)),
            ]
            + clip_scratch(len(clip_cols), clip_rows(w_clip.shape[0], n_tiles), factor.shape[1]),
        ),
        out_shape=[jax.ShapeDtypeStruct(out_shape, jnp.bfloat16), jax.ShapeDtypeStruct(w_clip.shape, jnp.bfloat16)],
        input_output_aliases=aliases,
        compiler_params=pltpu.CompilerParams(dimension_semantics=("arbitrary",), vmem_limit_bytes=VMEM_LIMIT),
        cost_estimate=pl.CostEstimate(
            flops=2 * n_chunks * rows * depth * width, bytes_accessed=2 * 2 * depth * width, transcendentals=0
        ),
    )(idx, *pieces, w_o, factor, w_clip, *aliased)


def solution(mesh):
    cp_size = mesh.shape["cp"]
    n_chips = cp_size // 2

    def permute(x, flip):
        return lax.ppermute(x, "cp", [(src, src ^ flip) for src in range(cp_size)])

    def device_body(hidden, pos_ids, w_q, w_k, w_v, w_o):
        cp_rank = lax.axis_index("cp")
        core, chip = cp_rank % 2, cp_rank // 2
        n_heads = w_q.shape[1] // HEAD_DIM
        half_heads = n_heads // 2
        half_tiles = half_heads * HEAD_DIM // TILE_N
        tiles_a = (half_tiles + 1) // 2
        heads_per_tile = TILE_N // HEAD_DIM
        groups = [(0, tiles_a), (tiles_a, half_tiles - tiles_a)]
        col_offs = tuple(t0 * TILE_N for t0, _ in groups)

        def index(*offsets):
            return jnp.stack([core] + [chip ^ d for d in offsets]).astype(jnp.int32)

        all_pos = lax.all_gather(pos_ids, "cp", tiled=True)
        cos_t, sin_t = (t.reshape(n_chips, -1, HEAD_DIM) for t in rope_tables(all_pos))

        same, other = {}, {}
        for d in range(n_chips):
            row = lax.dynamic_index_in_dim(hidden, chip ^ d, 0, keepdims=False)
            same[d] = permute(row, 2 * d) if d else row
            other[d] = permute(same[d], 1)

        def fill(qkv, offsets, tile0, n_tiles, *clip):
            pieces = [piece for d in offsets for piece in (same[d], other[d])]
            return project(index(*offsets), pieces, cos_t, sin_t, w_q, w_k, w_v, qkv, tile0, n_tiles, *clip)

        rest = tuple(range(1, n_chips))
        qkv = fill(None, (0,), 0, half_tiles)
        qkv = fill(qkv, rest[:-1], *groups[0])
        qkv = fill(qkv, rest[-1:], *groups[0])

        sent, maxes, factors, clip_cols = [], [], [], []
        for g, (tile0, n_tiles) in enumerate(groups):
            n_group = n_tiles * heads_per_tile
            if g == 1:
                *qkv, w_q_new, w_k_new = fill(qkv, rest, tile0, n_tiles, clip_cols[0], factors[0])
            vals, row_max = attend(*qkv, tile0 * heads_per_tile, n_group)
            local_max = jnp.max(row_max.reshape(n_group, -1), axis=1)
            spread = jnp.where(jnp.arange(2)[:, None] == core, local_max[None, :], -jnp.inf)
            every_max = lax.all_gather(spread, ("dp", "cp"))
            group_max = jnp.max(every_max, axis=0)
            maxes.append(group_max)
            factor = jnp.where(group_max > TAU_CLIP, jnp.sqrt(TAU_CLIP / group_max), 1.0)
            factors.append(jnp.repeat(factor, HEAD_DIM, axis=1))
            clip_cols.append(tuple((h * half_tiles + tile0) * TILE_N for h in range(2)))
            vals = vals.reshape(cp_size, -1, vals.shape[-1])
            got = {}
            for d in range(n_chips):
                for side in range(2):
                    piece = lax.dynamic_index_in_dim(vals, cp_rank ^ (2 * d + side), 0, keepdims=False)
                    got[d, side] = permute(piece, 2 * d + side) if d or side else piece
            sent.append(got)
        head_max = jnp.concatenate(maxes, axis=1).reshape(n_heads)

        def out_rows(offsets, w_clip, clip_into, into):
            pieces = [sent[g][d, side] for d in offsets for side in range(2) for g in range(len(groups))]
            return out_project(
                index(*offsets), pieces, col_offs, w_o, factors[1], w_clip, clip_into, clip_cols[1], into, hidden.shape
            )

        attn_out, w_q_new = out_rows((0,), w_q, w_q_new, None)
        attn_out, w_k_new = out_rows(rest, w_k, w_k_new, attn_out)
        return attn_out, head_max, w_q_new, w_k_new

    return jax.shard_map(
        device_body,
        mesh=mesh,
        in_specs=(P("dp", "cp", None), P("cp"), P(None, None), P(None, None), P(None, None), P(None, None)),
        out_specs=(P("dp", "cp", None), P(None), P(None, None), P(None, None)),
        check_vma=False,
    )
```

```python
import functools

import jax
import jax.numpy as jnp
from jax import lax
from jax.experimental import pallas as pl
from jax.experimental.pallas import tpu as pltpu
from jax.sharding import PartitionSpec as P


HEAD_DIM = 128
TAU_CLIP = 100.0
ROPE_THETA = 50000.0
TILE_N = 256
OUT_N = 512
SPLIT = 2
CLIP_ROWS = 64
LOG2_E = 1.4426950408889634
VMEM_LIMIT = 67043328


def rope_tables(pos_ids):
    half_dim = HEAD_DIM // 2
    inv_freq = jnp.float32(ROPE_THETA) ** (-jnp.arange(half_dim, dtype=jnp.float32) * (2.0 / HEAD_DIM))
    angle = pos_ids.astype(jnp.float32)[:, None] * inv_freq[None, :]
    cos_t, sin_t = jnp.cos(angle), jnp.sin(angle)
    return jnp.concatenate([cos_t, cos_t], axis=-1), jnp.concatenate([-sin_t, sin_t], axis=-1)


def clip_rows(total, n_steps):
    return -(-total // (16 * n_steps)) * 16


class ClipPass:
    def __init__(self, step, n_steps, units, fac_ref, buf, in_sems, out_sems):
        self.step, self.n_steps, self.units = step, n_steps, units
        self.fac_ref, self.buf, self.in_sems, self.out_sems = fac_ref, buf, in_sems, out_sems
        self.rows, self.width = buf.shape[2], buf.shape[3]

    def strip(self, ref, col0, step):
        row0 = pl.multiple_of(jnp.minimum(step * self.rows, ref.shape[0] - self.rows), 16)
        return ref.at[pl.ds(row0, self.rows), pl.ds(col0, self.width)]

    def copies(self, step, inward):
        slot = lax.rem(step, 3)
        for u, (src, dst, col0, _) in enumerate(self.units):
            if inward:
                yield pltpu.make_async_copy(self.strip(src, col0, step), self.buf.at[slot, u], self.in_sems.at[slot, u])
            else:
                yield pltpu.make_async_copy(self.buf.at[slot, u], self.strip(dst, col0, step), self.out_sems.at[slot, u])

    def start(self, step, inward):
        for copy in self.copies(step, inward):
            copy.start()

    def wait(self, step, inward):
        for copy in self.copies(step, inward):
            copy.wait()

    def open(self):
        step = self.step

        @pl.when(step == 0)
        def _():
            self.start(step, True)

        @pl.when(step >= 2)
        def _():
            self.wait(step - 2, False)

        @pl.when(step + 1 < self.n_steps)
        def _():
            self.start(step + 1, True)

        self.wait(step, True)

    def scale(self, u):
        slot, row = lax.rem(self.step, 3), self.units[u][3]
        for c0 in range(0, self.width, HEAD_DIM):
            fac = self.fac_ref[row : row + 1, c0 : c0 + HEAD_DIM]
            for r0 in range(0, self.rows, CLIP_ROWS):
                at = (slot, u, slice(r0, min(r0 + CLIP_ROWS, self.rows)), slice(c0, c0 + HEAD_DIM))
                self.buf[at] = (self.buf[at].astype(jnp.float32) * fac).astype(self.buf.dtype)

    def close(self):
        step = self.step
        self.start(step, False)

        @pl.when(step == self.n_steps - 1)
        def _():
            self.wait(step - 1, False)
            self.wait(step, False)


def clip_scratch(n_units, rows, width):
    return [
        pltpu.VMEM((3, n_units, rows, width), jnp.bfloat16),
        pltpu.SemaphoreType.DMA((3, n_units)),
        pltpu.SemaphoreType.DMA((3, n_units)),
    ]


def proj_kernel(n_chunks, n_alias, tile0, clip_cols, idx_ref, *refs):
    pieces = refs[: 2 * n_chunks]
    n_in = 2 * n_chunks + 5 + (1 if clip_cols else 0)
    cos_ref, sin_ref, wq_hbm, wk_hbm, wv_hbm = refs[2 * n_chunks : 2 * n_chunks + 5]
    outs = refs[n_in + n_alias :]
    (q_ref, k_ref, v_ref), outs = outs[:3], outs[3:]
    if clip_cols:
        (wq_new, wk_new), outs = outs[:2], outs[2:]
    (x_scr, x_sems, w_scr, w_sems), outs = outs[:4], outs[4:]
    tile, chunk = pl.program_id(0), pl.program_id(1)
    n_tiles = pl.num_programs(0)
    rows = pieces[0].shape[0]
    core = idx_ref[0]
    half_cols = wq_hbm.shape[1] // 2

    def piece_copies(c):
        part = rows // SPLIT
        for side in range(2):
            for n in range(SPLIT):
                row0 = (core if side == 0 else 1 - core) * rows + n * part
                yield pltpu.make_async_copy(
                    pieces[2 * c + side].at[pl.ds(n * part, part)],
                    x_scr.at[c, pl.ds(pl.multiple_of(row0, part), part)],
                    x_sems.at[c, side, n],
                )

    def weight_copies(at_tile):
        col0 = pl.multiple_of(core * half_cols + (tile0 + at_tile) * TILE_N, TILE_N)
        slot, part = lax.rem(at_tile, 2), wq_hbm.shape[0] // SPLIT
        for w, w_hbm in enumerate((wq_hbm, wk_hbm, wv_hbm)):
            for n in range(SPLIT):
                at = pl.ds(n * part, part)
                yield pltpu.make_async_copy(
                    w_hbm.at[at, pl.ds(col0, TILE_N)], w_scr.at[slot, w, at], w_sems.at[slot, w, n]
                )

    @pl.when(jnp.logical_and(tile == 0, chunk == 0))
    def _():
        for copy in piece_copies(0):
            copy.start()
        for copy in weight_copies(0):
            copy.start()
        for c in range(1, n_chunks):
            for copy in piece_copies(c):
                copy.start()

    for c in range(n_chunks):

        @pl.when(jnp.logical_and(tile == 0, chunk == c))
        def _():
            for copy in piece_copies(c):
                copy.wait()

    clip = None
    if clip_cols:
        units = [(src, dst, col0, h) for src, dst in ((wq_hbm, wq_new), (wk_hbm, wk_new)) for h, col0 in enumerate(clip_cols)]
        clip = ClipPass(tile * n_chunks + chunk, n_tiles * n_chunks, units, refs[2 * n_chunks + 5], *outs)
        clip.open()

    @pl.when(chunk == 0)
    def _():
        @pl.when(tile + 1 < n_tiles)
        def _():
            for copy in weight_copies(tile + 1):
                copy.start()

        for copy in weight_copies(tile):
            copy.wait()

    slot = lax.rem(tile, 2)
    x = x_scr[chunk]
    for w, o_ref in enumerate((q_ref, k_ref, v_ref)):
        acc = jnp.dot(x, w_scr[slot, w], preferred_element_type=jnp.float32)
        if w < 2:
            cos_t, sin_t = cos_ref[0], sin_ref[0]
            for h in range(TILE_N // HEAD_DIM):
                cols = slice(h * HEAD_DIM, (h + 1) * HEAD_DIM)
                t = acc[:, cols]
                o_ref[0, :, cols] = (t * cos_t + pltpu.roll(t, HEAD_DIM // 2, 1) * sin_t).astype(o_ref.dtype)
        else:
            o_ref[0] = acc.astype(o_ref.dtype)
        if clip:
            for u in range(len(clip.units)):
                if min(u, 2) == w:
                    clip.scale(u)

    if clip:
        clip.close()


def project(idx, pieces, cos_t, sin_t, w_q, w_k, w_v, into, tile0, n_tiles, clip_cols=(), factor=None):
    n_chunks = len(pieces) // 2
    rows, depth = pieces[0].shape
    total_chunks = cos_t.shape[0]
    half_cols = w_q.shape[1] // 2
    table_spec = pl.BlockSpec((1, 2 * rows, HEAD_DIM), lambda n, c, idx: (idx[1 + c], 0, 0))
    o_spec = pl.BlockSpec((1, 2 * rows, TILE_N), lambda n, c, idx: (idx[1 + c], 0, tile0 + n))
    any_spec = pl.BlockSpec(memory_space=pl.ANY)
    n_alias = 0 if into is None else 3
    o_shape = jax.ShapeDtypeStruct((total_chunks, 2 * rows, half_cols), jnp.bfloat16)
    flops = 2 * 3 * n_chunks * 2 * rows * depth * n_tiles * TILE_N
    first_alias = 1 + 2 * n_chunks + 5 + (1 if clip_cols else 0)
    scratch = [
        pltpu.VMEM((n_chunks, 2 * rows, depth), jnp.bfloat16),
        pltpu.SemaphoreType.DMA((n_chunks, 2, SPLIT)),
        pltpu.VMEM((2, 3, depth, TILE_N), jnp.bfloat16),
        pltpu.SemaphoreType.DMA((2, 3, SPLIT)),
    ]
    clip_specs, clip_args, clip_outs = [], [], []
    if clip_cols:
        clip_specs = [pl.BlockSpec(factor.shape, lambda n, c, idx: (0, 0))]
        clip_args = [factor]
        clip_outs = [jax.ShapeDtypeStruct(w_q.shape, w_q.dtype)] * 2
        scratch += clip_scratch(2 * len(clip_cols), clip_rows(depth, n_tiles * n_chunks), factor.shape[1])
    return pl.pallas_call(
        functools.partial(proj_kernel, n_chunks, n_alias, tile0, clip_cols),
        grid_spec=pltpu.PrefetchScalarGridSpec(
            num_scalar_prefetch=1,
            grid=(n_tiles, n_chunks),
            in_specs=[any_spec] * (2 * n_chunks) + [table_spec] * 2 + [any_spec] * 3 + clip_specs + [any_spec] * n_alias,
            out_specs=[o_spec] * 3 + [any_spec] * len(clip_outs),
            scratch_shapes=scratch,
        ),
        out_shape=[o_shape] * 3 + clip_outs,
        input_output_aliases={first_alias + i: i for i in range(n_alias)},
        compiler_params=pltpu.CompilerParams(
            dimension_semantics=("arbitrary", "arbitrary"), vmem_limit_bytes=VMEM_LIMIT
        ),
        cost_estimate=pl.CostEstimate(
            flops=flops, bytes_accessed=2 * 3 * depth * n_tiles * TILE_N + 2 * n_chunks * rows * depth * 2, transcendentals=0
        ),
    )(idx, *pieces, cos_t, sin_t, w_q, w_k, w_v, *clip_args, *(into or ()))


def attn_kernel(blk, rank_ref, q_ref, k_ref, v_ref, *refs):
    *o_refs, m_ref, s_scr, p_scr, o_scr = refs
    n_chunks, rows, _ = q_ref.shape
    per_chunk = rows // blk
    n_blocks = n_chunks * per_chunk
    scale = HEAD_DIM ** -0.5
    lanes = blk // HEAD_DIM if blk >= HEAD_DIM else 1
    width = blk // lanes
    causal = lax.broadcasted_iota(jnp.int32, (blk, blk), 0) >= lax.broadcasted_iota(jnp.int32, (blk, blk), 1)

    def rows_of(ref, i):
        r0 = (i % per_chunk) * blk
        return ref[i // per_chunk, r0 : r0 + blk, :]

    def scores(i):
        q = rows_of(q_ref, i)
        lane_max = None
        for j in range(i + 1):
            s = lax.dot_general(q, rows_of(k_ref, j), (((1,), (1,)), ((), ())), preferred_element_type=jnp.float32)
            if j == i:
                s = jnp.where(causal, s, -jnp.inf)
            s_scr[i % 2, :, j * blk : (j + 1) * blk] = s
            for c in range(lanes):
                part = s[:, c * width : (c + 1) * width]
                lane_max = part if lane_max is None else jnp.maximum(lane_max, part)
        return jnp.max(lane_max, axis=-1, keepdims=True)

    row_max = scores(0)
    head_max = row_max
    for i in range(n_blocks):
        if i + 1 < n_blocks:
            next_max = scores(i + 1)
            head_max = jnp.maximum(head_max, next_max)
        lane_sum = None
        for j in range(i + 1):
            cols = slice(j * blk, (j + 1) * blk)
            p = jnp.exp2((s_scr[i % 2, :, cols] - row_max) * (scale * LOG2_E))
            for c in range(lanes):
                part = p[:, c * width : (c + 1) * width]
                lane_sum = part if lane_sum is None else lane_sum + part
            p_scr[i % 2, :, cols] = p.astype(p_scr.dtype)
        keys = (i + 1) * blk
        values = v_ref[...].reshape(n_chunks * rows, HEAD_DIM)[:keys]
        acc = jnp.dot(p_scr[i % 2, :, :keys], values, preferred_element_type=jnp.float32)
        row_sum = jnp.sum(lane_sum, axis=-1, keepdims=True)
        o_scr[i] = (acc / row_sum).astype(o_scr.dtype)
        if i + 1 < n_blocks:
            row_max = next_max
    for flip, o_ref in enumerate(o_refs):
        o_ref[...] = o_scr[lax.bitwise_xor(rank_ref[0], flip)]
    m_ref[...] = jnp.broadcast_to(jnp.max(head_max, axis=0, keepdims=True) * scale, m_ref.shape)


def attend(rank, q, k, v, head0, n_heads):
    n_chunks, rows, _ = q.shape
    blk = rows // 2
    n_blocks = 2 * n_chunks
    seq = n_chunks * rows
    in_spec = pl.BlockSpec((n_chunks, rows, HEAD_DIM), lambda h, rank: (0, 0, head0 + h))
    o_spec = pl.BlockSpec((blk, HEAD_DIM), lambda h, rank: (0, h))
    return pl.pallas_call(
        functools.partial(attn_kernel, blk),
        grid_spec=pltpu.PrefetchScalarGridSpec(
            num_scalar_prefetch=1,
            grid=(n_heads,),
            in_specs=[in_spec] * 3,
            out_specs=[o_spec] * n_blocks + [pl.BlockSpec((8, HEAD_DIM), lambda h, rank: (h, 0))],
            scratch_shapes=[
                pltpu.VMEM((2, blk, seq), jnp.float32),
                pltpu.VMEM((2, blk, seq), jnp.bfloat16),
                pltpu.VMEM((n_blocks, blk, HEAD_DIM), jnp.bfloat16),
            ],
        ),
        out_shape=[jax.ShapeDtypeStruct((blk, n_heads * HEAD_DIM), jnp.bfloat16)] * n_blocks
        + [jax.ShapeDtypeStruct((8 * n_heads, HEAD_DIM), jnp.float32)],
        compiler_params=pltpu.CompilerParams(dimension_semantics=("arbitrary",), vmem_limit_bytes=VMEM_LIMIT),
        cost_estimate=pl.CostEstimate(
            flops=8 * seq * seq * HEAD_DIM * n_heads // 2,
            bytes_accessed=8 * seq * HEAD_DIM * n_heads,
            transcendentals=seq * seq * n_heads // 2,
        ),
    )(rank, q, k, v)


def out_kernel(n_chunks, col_offs, n_alias, clip_cols, idx_ref, *refs):
    n_groups = len(col_offs)
    n_pieces = n_chunks * 2 * n_groups
    pieces = refs[:n_pieces]
    wo_ref, fac_ref, wc_hbm = refs[n_pieces : n_pieces + 3]
    o_hbm, c_hbm, a_scr, o_scr, a_sems, o_sems, *clip_refs = refs[n_pieces + 3 + n_alias :]
    tile, n_tiles = pl.program_id(0), pl.num_programs(0)
    core = idx_ref[0]
    rows = pieces[0].shape[0]
    half_cols = a_scr.shape[1] // 2

    def piece_copies():
        copies = []
        for c in range(n_chunks):
            for side in range(2):
                for g in range(n_groups):
                    n = (c * 2 + side) * n_groups + g
                    col0 = (core if side == 0 else 1 - core) * half_cols + col_offs[g]
                    width = pieces[n].shape[1]
                    copies.append(
                        pltpu.make_async_copy(
                            pieces[n],
                            a_scr.at[pl.ds(c * rows, rows), pl.ds(pl.multiple_of(col0, HEAD_DIM), width)],
                            a_sems.at[n],
                        )
                    )
        return copies

    def out_copies(slot, at_tile):
        return [
            pltpu.make_async_copy(
                o_scr.at[slot, pl.ds(c * rows, rows)],
                o_hbm.at[idx_ref[1 + c], :, pl.ds(pl.multiple_of(at_tile * OUT_N, OUT_N), OUT_N)],
                o_sems.at[slot, c],
            )
            for c in range(n_chunks)
        ]

    @pl.when(tile == 0)
    def _():
        for copy in piece_copies():
            copy.start()

    clip = ClipPass(tile, n_tiles, [(wc_hbm, c_hbm, col0, h) for h, col0 in enumerate(clip_cols)], fac_ref, *clip_refs)
    clip.open()

    @pl.when(tile == 0)
    def _():
        for copy in piece_copies():
            copy.wait()

    slot = lax.rem(tile, 2)

    @pl.when(tile >= 2)
    def _():
        for copy in out_copies(slot, tile - 2):
            copy.wait()

    a = a_scr[...]
    for c0 in range(0, OUT_N, TILE_N):
        cols = slice(c0, c0 + TILE_N)
        o_scr[slot, :, cols] = jnp.dot(a, wo_ref[:, cols], preferred_element_type=jnp.float32).astype(o_scr.dtype)
    for u in range(len(clip.units)):
        clip.scale(u)
    for copy in out_copies(slot, tile):
        copy.start()
    clip.close()

    @pl.when(tile == n_tiles - 1)
    def _():
        for copy in out_copies(1 - slot, tile - 1):
            copy.wait()
        for copy in out_copies(slot, tile):
            copy.wait()


def out_project(idx, pieces, col_offs, w_o, factor, w_clip, clip_into, clip_cols, into, out_shape):
    n_groups = len(col_offs)
    n_chunks = len(pieces) // (2 * n_groups)
    rows = pieces[0].shape[0]
    depth, width = w_o.shape
    n_tiles = width // OUT_N
    any_spec = pl.BlockSpec(memory_space=pl.ANY)
    tile_spec = pl.BlockSpec((depth, OUT_N), lambda n, idx: (0, n))
    alias_at = 1 + len(pieces) + 3
    aliased, aliases = [clip_into], {alias_at: 1}
    if into is not None:
        aliased, aliases = [clip_into, into], {alias_at: 1, alias_at + 1: 0}
    return pl.pallas_call(
        functools.partial(out_kernel, n_chunks, col_offs, len(aliased), clip_cols),
        grid_spec=pltpu.PrefetchScalarGridSpec(
            num_scalar_prefetch=1,
            grid=(n_tiles,),
            in_specs=[any_spec] * len(pieces)
            + [tile_spec, pl.BlockSpec(factor.shape, lambda n, idx: (0, 0)), any_spec]
            + [any_spec] * len(aliased),
            out_specs=[any_spec, any_spec],
            scratch_shapes=[
                pltpu.VMEM((n_chunks * rows, depth), jnp.bfloat16),
                pltpu.VMEM((2, n_chunks * rows, OUT_N), jnp.bfloat16),
                pltpu.SemaphoreType.DMA((len(pieces),)),
                pltpu.SemaphoreType.DMA((2, n_chunks)),
            ]
            + clip_scratch(len(clip_cols), clip_rows(w_clip.shape[0], n_tiles), factor.shape[1]),
        ),
        out_shape=[jax.ShapeDtypeStruct(out_shape, jnp.bfloat16), jax.ShapeDtypeStruct(w_clip.shape, jnp.bfloat16)],
        input_output_aliases=aliases,
        compiler_params=pltpu.CompilerParams(dimension_semantics=("arbitrary",), vmem_limit_bytes=VMEM_LIMIT),
        cost_estimate=pl.CostEstimate(
            flops=2 * n_chunks * rows * depth * width, bytes_accessed=2 * 2 * depth * width, transcendentals=0
        ),
    )(idx, *pieces, w_o, factor, w_clip, *aliased)


def solution(mesh):
    cp_size = mesh.shape["cp"]
    n_chips = cp_size // 2

    def permute(x, flip):
        return lax.ppermute(x, "cp", [(src, src ^ flip) for src in range(cp_size)])

    def device_body(hidden, pos_ids, w_q, w_k, w_v, w_o):
        cp_rank = lax.axis_index("cp")
        core, chip = cp_rank % 2, cp_rank // 2
        n_heads = w_q.shape[1] // HEAD_DIM
        half_heads = n_heads // 2
        half_tiles = half_heads * HEAD_DIM // TILE_N
        tiles_a = (half_tiles + 1) // 2
        heads_per_tile = TILE_N // HEAD_DIM
        groups = [(0, tiles_a), (tiles_a, half_tiles - tiles_a)]
        col_offs = tuple(t0 * TILE_N for t0, _ in groups)

        def index(*offsets):
            return jnp.stack([core] + [chip ^ d for d in offsets]).astype(jnp.int32)

        all_pos = lax.all_gather(pos_ids, "cp", tiled=True)
        cos_t, sin_t = (t.reshape(n_chips, -1, HEAD_DIM) for t in rope_tables(all_pos))

        same, other = {}, {}
        for d in range(n_chips):
            row = lax.dynamic_index_in_dim(hidden, chip ^ d, 0, keepdims=False)
            same[d] = permute(row, 2 * d) if d else row
            other[d] = permute(same[d], 1)

        def fill(qkv, offsets, tile0, n_tiles, *clip):
            pieces = [piece for d in offsets for piece in (same[d], other[d])]
            return project(index(*offsets), pieces, cos_t, sin_t, w_q, w_k, w_v, qkv, tile0, n_tiles, *clip)

        rest = tuple(range(1, n_chips))
        qkv = fill(None, (0,), 0, half_tiles)
        qkv = fill(qkv, rest[:-1], *groups[0])
        qkv = fill(qkv, rest[-1:], *groups[0])

        sent, maxes, factors, clip_cols = [], [], [], []
        for g, (tile0, n_tiles) in enumerate(groups):
            n_group = n_tiles * heads_per_tile
            if g == 1:
                *qkv, w_q_new, w_k_new = fill(qkv, rest, tile0, n_tiles, clip_cols[0], factors[0])
            *vals, row_max = attend(cp_rank.astype(jnp.int32)[None], *qkv, tile0 * heads_per_tile, n_group)
            local_max = jnp.max(row_max.reshape(n_group, -1), axis=1)
            spread = jnp.where(jnp.arange(2)[:, None] == core, local_max[None, :], -jnp.inf)
            every_max = lax.all_gather(spread, ("dp", "cp"))
            group_max = jnp.max(every_max, axis=0)
            maxes.append(group_max)
            factor = jnp.where(group_max > TAU_CLIP, jnp.sqrt(TAU_CLIP / group_max), 1.0)
            factors.append(jnp.repeat(factor, HEAD_DIM, axis=1))
            clip_cols.append(tuple((h * half_tiles + tile0) * TILE_N for h in range(2)))
            got = {}
            for flip, piece in enumerate(vals):
                at = divmod(flip, 2)
                got[at] = permute(piece, flip) if flip else piece
            sent.append(got)
        head_max = jnp.concatenate(maxes, axis=1).reshape(n_heads)

        def out_rows(offsets, w_clip, clip_into, into):
            pieces = [sent[g][d, side] for d in offsets for side in range(2) for g in range(len(groups))]
            return out_project(
                index(*offsets), pieces, col_offs, w_o, factors[1], w_clip, clip_into, clip_cols[1], into, hidden.shape
            )

        attn_out, w_q_new = out_rows((0,), w_q, w_q_new, None)
        attn_out, w_k_new = out_rows(rest, w_k, w_k_new, attn_out)
        return attn_out, head_max, w_q_new, w_k_new

    return jax.shard_map(
        device_body,
        mesh=mesh,
        in_specs=(P("dp", "cp", None), P("cp"), P(None, None), P(None, None), P(None, None), P(None, None)),
        out_specs=(P("dp", "cp", None), P(None), P(None, None), P(None, None)),
        check_vma=False,
    )
```
